256 devices in a mesh: row: 32 (over z, x), col: 8 (over y, core).
Axes of the slice: x: 4, y: 4, z: 8, core: 2. Of those that a mesh axis runs over, the one named last changes fastest.
Arguments:
- integrals: bfloat16 [65536, 8192], P('row', 'col'), may hold values from -0.0234375 to 0.0234375
- lambda2: bfloat16 [2016, 65536], P('col', 'row'), may hold values from -6 to 6
- source_terms: float32 [2016, 8192], P('row', 'col'), may hold values from -6 to 6
- hist_amp: bfloat16 [5, 2016, 8192], P(None, 'row', 'col'), may hold values from -6 to 6
- hist_err: bfloat16 [5, 2016, 8192], P(None, 'row', 'col'), may hold values from -64 to 64
- eps_occ: float32 [64], replicated, may hold values from -1 to -0.3
- eps_vir: float32 [800], replicated, may hold values from 0.1 to 1
- occ_pair: int32 [2, 2016], P(None, 'row'), may hold values from 0 to 63, as said below
- vir_pair: int32 [2, 8192], P(None, 'col'), may hold values from 0 to 799, as said below
Outputs:
- updated: float32 [2016, 8192], P('row', 'col')
The draws below stay inside these ranges and needn't reach their ends.
Inputs may be any that keep to these rules, and one draw needn't show every extreme that they name: `occ_pair`: every pair i < j of the 64 occupied orbitals appears exactly once, in some order. `vir_pair`: in every column the first orbital is smaller than the second.
All inputs are finite; a program needn't handle non-finite values.
Results may differ from the reference program's by a relative error of at most 0.0003.
Values may be sent and summed in bfloat16 or wider, within the bound.
A program may use at most 64 MiB of HBM per device.

```python
import math
import jax
import jax.numpy as jnp
import numpy as np
from jax import lax

NOCC = 64
NVIR = 800
IJ = 2016
NHIST = 5
CD = 65536
AB = 8192


def draw_occ_pair(key, part):
    pairs = np.triu_indices(NOCC, 1)
    table = jnp.asarray(np.stack(pairs).astype(np.int32))
    order = jax.random.permutation(key, IJ)
    return table[:, order].astype(jnp.int32)


def draw_vir_pair(key, part):
    first_key, second_key = jax.random.split(jax.random.fold_in(key, 17))
    lower = jax.random.randint(first_key, (AB,), 0, NVIR - 1, dtype=jnp.int32)
    offsets = jax.random.randint(second_key, (AB,), 0, 1 << 20, dtype=jnp.int32)
    upper = lower + 1 + offsets % (NVIR - 1 - lower)
    return jnp.stack([lower, upper]).astype(jnp.int32)


def draw_hist_err(key, part):
    keys = jax.random.split(jax.random.fold_in(key, 29), 4)
    row_pos = jnp.arange(IJ, dtype=jnp.float32) / IJ
    col_pos = jnp.arange(AB, dtype=jnp.float32) / AB
    row_scale = jnp.exp(jax.random.uniform(keys[0], (IJ,), jnp.float32) * math.log(10.0)) * (1.0 + 2.0 * row_pos) / 8.0
    col_scale = jnp.exp(jax.random.uniform(keys[1], (AB,), jnp.float32) * math.log(10.0)) * (1.0 + 2.0 * col_pos) / 8.0
    common = jnp.clip(jax.random.normal(keys[2], (IJ, AB), jnp.float32), -6.0, 6.0)
    own = jnp.clip(jax.random.normal(keys[3], (NHIST, IJ, AB), jnp.float32), -6.0, 6.0)
    mixing = 0.6
    level = 1.2
    values = (mixing * common[None] + math.sqrt(1.0 - mixing * mixing) * own) * (row_scale[:, None] * col_scale[None, :])[None]
    return jnp.clip(level * values, -64.0, 64.0).astype(jnp.bfloat16)


def spiked(entries, stream_key, source, target, shards_of, factor):
    owner, partner = [(jnp.arange(entries.shape[dim]) // (entries.shape[dim] // shards_of)).reshape([-1 if axis == dim else 1 for axis in range(entries.ndim)]) for dim in (source, target)]
    chosen = jax.random.permutation(stream_key, shards_of)[partner]
    strong = (owner == chosen) | (owner == (partner + shards_of // 2) % shards_of)
    return jnp.where(strong, factor * entries, entries)


def level_of(own_key, dims, cuts, smallest, top_value):
    level, own = 1.0, jax.random.fold_in(own_key, 6)
    for dim, parts in cuts:
        steps = jnp.exp(jax.random.uniform(jax.random.fold_in(own, dim), (parts,), jnp.float32, smallest / len(cuts), top_value / len(cuts)))
        level = level * jnp.repeat(steps, dims[dim] // parts).reshape([-1 if axis == dim else 1 for axis in range(len(dims))])
    return level


def scatter_about(stream_key, shape, deviation, limit, cuts=(), kind=jnp.bfloat16):
    entries = deviation * jax.random.normal(stream_key, shape, jnp.float32)
    if cuts:
        entries = entries * level_of(stream_key, shape, cuts, -0.22, 0.18)
    return jnp.clip(entries, -limit, limit).astype(kind)


def gaussian_with(key, dims, scale, limit, cuts, heavy, kind=jnp.bfloat16):
    entries = scale * jax.random.normal(key, dims, jnp.float32)
    if cuts:
        entries = entries * level_of(key, dims, cuts, -0.22, 0.18)
    return jnp.clip(spiked(entries, jax.random.fold_in(key, 3), *heavy), -limit, limit).astype(kind)


def setup_inputs(seed: int = 0) -> dict:
    key_of = jax.random.split(jax.random.key(seed), 10)
    integrals = scatter_about(key_of[0], (CD, AB), CD ** -0.5, 0.0234375, ((0, 32), (1, 8)))
    lambda2 = gaussian_with(key_of[1], (IJ, CD), 1.0, 6.0, ((0, 8), (1, 32)), (1, 0, 32, 2.75))
    source_terms = scatter_about(key_of[2], (IJ, AB), 1.0, 6.0, ((0, 32), (1, 8)), jnp.float32)
    hist_amp = scatter_about(key_of[3], (NHIST, IJ, AB), 1.0, 6.0, ((1, 32), (2, 8)))
    hist_err = draw_hist_err(jax.random.fold_in(key_of[9], 71), 0)
    eps_occ = jnp.clip(jax.random.uniform(key_of[5], (NOCC,), jnp.float32, -1.0, -0.3), -1.0, -0.3)
    eps_vir = jnp.clip(jax.random.uniform(key_of[6], (NVIR,), jnp.float32, 0.1, 1.0), 0.1, 1.0)
    occ_pair = draw_occ_pair(jax.random.fold_in(key_of[9], 71), 0)
    vir_pair = draw_vir_pair(jax.random.fold_in(key_of[9], 71), 0)
    return {"integrals": integrals, "lambda2": lambda2, "source_terms": source_terms, "hist_amp": hist_amp, "hist_err": hist_err, "eps_occ": eps_occ, "eps_vir": eps_vir, "occ_pair": occ_pair, "vir_pair": vir_pair}


precise = lax.Precision.HIGHEST

def pair_energy(pairs, energies):
    levels = jnp.arange(energies.shape[0], dtype=jnp.int32)
    first = jnp.sum(jnp.where(pairs[0][:, None] == levels[None, :], energies[None, :], 0.0), axis=1)
    second = jnp.sum(jnp.where(pairs[1][:, None] == levels[None, :], energies[None, :], 0.0), axis=1)
    return first + second

def diis_weights(correlation):
    factor = jnp.linalg.cholesky(correlation)
    order = correlation.shape[0]
    forward = []
    for k in range(order):
        running = jnp.ones((), correlation.dtype)
        for m in range(k):
            running = running - factor[k, m] * forward[m]
        forward.append(running / factor[k, k])
    backward = [None] * order
    for k in reversed(range(order)):
        running = forward[k]
        for m in range(k + 1, order):
            running = running - factor[m, k] * backward[m]
        backward[k] = running / factor[k, k]
    solved = jnp.stack(backward)
    return solved / jnp.sum(solved)

def reference(integrals, lambda2, source_terms, hist_amp, hist_err, eps_occ, eps_vir, occ_pair, vir_pair):
    ladder = jnp.dot(lambda2.astype(jnp.float32), integrals.astype(jnp.float32), preferred_element_type=jnp.float32)
    denominator = pair_energy(occ_pair, eps_occ)[:, None] - pair_energy(vir_pair, eps_vir)[None, :]
    raw_update = (source_terms + ladder) / denominator
    err_new = raw_update - hist_amp[0].astype(jnp.float32)
    stored_count = hist_err.shape[0]
    stacked = jnp.concatenate([hist_err.astype(jnp.float32).reshape(stored_count, -1), err_new.reshape(1, -1)], axis=0)
    correlation = jnp.dot(stacked, stacked.T, precision=precise)
    weights = diis_weights(correlation)
    updated = weights[stored_count] * raw_update
    for k in range(stored_count):
        updated = updated + weights[k] * hist_amp[k].astype(jnp.float32)
    return updated
```

```python
import functools

import jax
import jax.numpy as jnp
from jax import lax
from jax.experimental import pallas as pl
from jax.experimental.pallas import tpu as pltpu
from jax.sharding import PartitionSpec as P

MESH = pl.DeviceIdType.MESH
F32 = jnp.float32
BF16 = jnp.bfloat16
LEVELS = 32000.0

NX, NY, NZ = 4, 4, 8
ROWS, COLS = NX * NZ, NY * 2
BLOCK = 63
SUB = 16
PIECES = 4
KDIM = 2048
NDIM = 1024
NT = NDIM // 128

ORDER = (
    ("own", 0), ("sib", 0), ("near", 0), ("near", 1), ("far", 0),
    ("near", 2), ("far", 1), ("near", 3), ("far", 2), ("far", 3),
)
GROUPS = len(ORDER)
SIZES = tuple(2 if kind == "far" else 4 for kind, _ in ORDER)
ZBASE = tuple(sum(SIZES[:g]) for g in range(GROUPS))
ZSENDS = sum(SIZES)


def rows_of(piece):
    return SUB if piece < PIECES - 1 else BLOCK - SUB * (PIECES - 1)


def widen(row, count):
    return jnp.concatenate([row] * count, axis=1)


def fold(values, op):
    out = values[:, 0:128]
    for j in range(1, values.shape[1] // 128):
        out = op(out, values[:, 128 * j : 128 * (j + 1)])
    return out


def encode(values):
    top = jnp.max(fold(jnp.abs(values), jnp.maximum), axis=0, keepdims=True)
    top = jnp.maximum(top, 1e-30)
    factor = widen(LEVELS / top, values.shape[1] // 128)
    code = jnp.round(values * factor).astype(jnp.int32).astype(jnp.int16)
    return code, top * (1.0 / LEVELS)


def decode(code, scale):
    return code.astype(jnp.int32).astype(F32) * widen(scale, code.shape[1] // 128)


def split3(values):
    high = values.astype(BF16)
    rest = values - high.astype(F32)
    middle = rest.astype(BF16)
    low = (rest - middle.astype(F32)).astype(BF16)
    return high, middle, low


def lane_sums(values):
    return jnp.sum(fold(values, jnp.add), axis=0, keepdims=True)


def solve(corr):
    factor = [[None] * 6 for _ in range(6)]
    for j in range(6):
        for i in range(j, 6):
            run = corr[i][j]
            for k in range(j):
                run = run - factor[i][k] * factor[j][k]
            if i == j:
                factor[j][j] = jnp.sqrt(run)
            else:
                factor[i][j] = run / factor[j][j]
    forward = []
    for k in range(6):
        run = jnp.ones_like(corr[0][0])
        for m in range(k):
            run = run - factor[k][m] * forward[m]
        forward.append(run / factor[k][k])
    back = [None] * 6
    for k in reversed(range(6)):
        run = forward[k]
        for m in range(k + 1, 6):
            run = run - factor[m][k] * back[m]
        back[k] = run / factor[k][k]
    total = back[0]
    for k in range(1, 6):
        total = total + back[k]
    return [b / total for b in back]


def kernel(
    ints_hbm, lam_hbm, src_hbm, amp_hbm, err_hbm, eocc_hbm, evir_hbm, occ_hbm, vir_hbm,
    out_ref,
    ints, lam, src, amp, err, eocc, evir, occ, vir,
    a_own, a_sib, a_near, a_far, part,
    xa_out, xa_in, xas_out, xas_in, xb_out, xb_in, xbs_out, xbs_in,
    z_out, z_in, zs_out, zs_in, z_own,
    raw_buf, up, vq, corr_h, corr_n, sum_h, sum_n, h1_in, h2_in, n1_in, n2_in,
    load_sem, ag_send, ag_recv, xa_s, xa_r, xas_s, xas_r, xb_s, xb_r, xbs_s, xbs_r,
    z_s, zs_s, z_r, zs_r, c_s, c_r,
):
    row = lax.axis_index("row")
    col = lax.axis_index("col")
    z, x = row // NX, row % NX
    y, core = col // 2, col % 2
    sib = 1 - core
    xp, xm, xo = (x + 1) % NX, (x + 3) % NX, (x + 2) % NX
    yp, ym = (y + 1) % NY, (y + 3) % NY

    def at_y(yy):
        return (row, yy * 2 + core)

    def at_x(xx):
        return (z * NX + xx, col)

    twin = (row, y * 2 + sib)

    barrier = pltpu.get_barrier_semaphore()

    def greet_rows(o, carry):
        pl.semaphore_signal(barrier, inc=1, device_id=((row + o) % ROWS, col), device_id_type=MESH)
        return carry

    def greet_cols(o, carry):
        pl.semaphore_signal(barrier, inc=1, device_id=(row, (col + o) % COLS), device_id_type=MESH)
        return carry

    lax.fori_loop(1, COLS, greet_cols, 0)
    lax.fori_loop(1, ROWS, greet_rows, 0)

    loads = [
        pltpu.make_async_copy(s, d, load_sem.at[i])
        for i, (s, d) in enumerate(
            (
                (lam_hbm, lam), (ints_hbm, ints), (eocc_hbm, eocc), (evir_hbm, evir),
                (occ_hbm, occ), (vir_hbm, vir), (err_hbm, err), (src_hbm, src), (amp_hbm, amp),
            )
        )
    ]
    for load in loads:
        load.start()

    loads[0].wait()
    r_id = lax.broadcasted_iota(jnp.int32, (256, 252), 0)
    s_id = lax.broadcasted_iota(jnp.int32, (256, 252), 1)
    inner = (r_id // 64) * SUB + r_id % SUB
    source = ((r_id % 64) // SUB) * BLOCK + inner
    pick = jnp.where((source == s_id) & (inner < BLOCK), 1.0, 0.0).astype(BF16)

    def permute(t, carry):
        cols = pl.ds(pl.multiple_of(t * 512, 512), 512)
        a_own[:, cols] = jnp.dot(pick, lam[:, cols], preferred_element_type=F32).astype(BF16)
        return carry

    lax.fori_loop(0, KDIM // 512, permute, 0)

    def remote(src_ref, dst_ref, ssem, rsem, dev):
        return pltpu.make_async_remote_copy(
            src_ref=src_ref, dst_ref=dst_ref, send_sem=ssem, recv_sem=rsem,
            device_id=dev, device_id_type=MESH,
        )

    def ag(kind, p, s, d, dev):
        k = kind * PIECES + p
        return remote(s, d, ag_send.at[k], ag_recv.at[k], dev)

    def piece_of(ref, p):
        return ref.at[pl.ds(64 * p, 64)]

    def near(p, slot):
        return a_near.at[p, pl.ds(64 * slot, 64)]

    def far(p, slot, half):
        return a_far.at[p, pl.ds(64 * slot + 32 * half, 32)]

    own_up = [ag(0, p, piece_of(a_own, p), near(p, 0), at_y(yp)) for p in range(PIECES)]
    own_down = [ag(1, p, piece_of(a_own, p), near(p, 1), at_y(ym)) for p in range(PIECES)]
    own_twin = [ag(2, p, piece_of(a_own, p), piece_of(a_sib, p), twin) for p in range(PIECES)]
    fwd_up = [
        ag(3, p, a_near.at[p, pl.ds(0, 32)], far(p, 0, 0), at_y(yp)) for p in range(PIECES)
    ]
    fwd_down = [
        ag(4, p, a_near.at[p, pl.ds(96, 32)], far(p, 0, 1), at_y(ym)) for p in range(PIECES)
    ]
    near_twin = [
        [ag(5 + s, p, near(p, s), near(p, 2 + s), twin) for p in range(PIECES)] for s in range(2)
    ]
    far_twin = [
        [ag(7 + h, p, far(p, 0, h), far(p, 1, h), twin) for p in range(PIECES)] for h in range(2)
    ]

    def multiply(g):
        kind, p = ORDER[g]
        n = SIZES[g]
        a = {"own": a_own, "sib": a_sib}.get(kind)
        if a is None:
            a = a_near.at[p] if kind == "near" else a_far.at[p]

        def tile(t, carry):
            cols = pl.ds(pl.multiple_of(t * 256, 256), 256)
            res = jnp.dot(a[...], ints[:, cols], preferred_element_type=F32)
            part[g, 0:n, :, :, cols] = res.reshape(n, NX, SUB, 256)
            return carry

        lax.fori_loop(0, NDIM // 256, tile, 0)

    def xmsg(out, inn, ss, rs, g, d, dev, cut):
        n = SIZES[g]
        s = out.at[g, d, pl.ds(0, n)] if cut else out.at[g, d]
        t = inn.at[g, d, pl.ds(0, n)] if cut else inn.at[g, d]
        return remote(s, t, ss.at[g, d], rs.at[g, d], dev)

    sides = (xp, xm)
    xa = [[xmsg(xa_out, xa_in, xa_s, xa_r, g, d, at_x(sides[d]), True) for d in range(2)] for g in range(GROUPS)]
    xas = [[xmsg(xas_out, xas_in, xas_s, xas_r, g, d, at_x(sides[d]), False) for d in range(2)] for g in range(GROUPS)]
    xb = [[xmsg(xb_out, xb_in, xb_s, xb_r, g, d, at_x(sides[d]), True) for d in range(2)] for g in range(GROUPS)]
    xbs = [[xmsg(xbs_out, xbs_in, xbs_s, xbs_r, g, d, at_x(sides[d]), False) for d in range(2)] for g in range(GROUPS)]

    def stage_a(g):
        def block(i, carry):
            for d in range(2):
                code, scale = encode(part[g, i, xo, :, 512 * d : 512 * (d + 1)])
                xa_out[g, d, i] = code
                xas_out[g, d, pl.ds(i, 1), :] = scale
            return carry

        lax.fori_loop(0, SIZES[g], block, 0)
        for d in range(2):
            xa[g][d].start()
            xas[g][d].start()

    def stage_b(g):
        for d in range(2):
            xa[g][d].wait_recv()
            xas[g][d].wait_recv()

        def block(i, carry):
            for d in range(2):
                mine = part[g, i, sides[d]]
                got = decode(xa_in[g, d, i], xas_in[g, d, pl.ds(i, 1), :])
                if d == 0:
                    both = jnp.concatenate([mine[:, :512] + got, mine[:, 512:]], axis=1)
                else:
                    both = jnp.concatenate([mine[:, :512], mine[:, 512:] + got], axis=1)
                code, scale = encode(both)
                xb_out[g, d, i] = code
                xbs_out[g, d, pl.ds(i, 1), :] = scale
            return carry

        lax.fori_loop(0, SIZES[g], block, 0)
        for d in range(2):
            xb[g][d].start()
            xbs[g][d].start()

    def place(g, i):
        kind, p = ORDER[g]
        if kind == "own":
            return col, i
        if kind == "sib":
            return y * 2 + sib, i
        if kind == "near":
            return ((y + 3 + 2 * (i % 2)) % NY) * 2 + (core + i // 2) % 2, p
        return ((y + 2) % NY) * 2 + (core + i) % 2, p

    def zmsg(g, i):
        owner, p = place(g, i)
        k = ZBASE[g] + i
        slot = (z - owner + NZ - 1) % NZ
        dev = (owner * NX + x, col)
        return (
            owner,
            p,
            remote(z_out.at[k], z_in.at[p, slot], z_s.at[k], z_r.at[p], dev),
            remote(zs_out.at[k], zs_in.at[p, slot], zs_s.at[k], zs_r.at[p], dev),
        )

    def stage_c(g):
        for d in range(2):
            xb[g][d].wait_recv()
            xbs[g][d].wait_recv()

        def block(i, carry):
            k = ZBASE[g] + i
            owner, p, data, scales = zmsg(g, i)
            total = part[g, i, x]
            for d in range(2):
                total = total + decode(xb_in[g, d, i], xbs_in[g, d, pl.ds(i, 1), :])

            @pl.when(owner == z)
            def _():
                z_own[p] = total

            @pl.when(owner != z)
            def _():
                code, scale = encode(total)
                z_out[k] = code
                zs_out[k, 0:1, :] = scale
                data.start()
                scales.start()

            return carry

        lax.fori_loop(0, SIZES[g], block, 0)

    def finish_sends(g):
        for d in range(2):
            xa[g][d].wait_send()
            xas[g][d].wait_send()
            xb[g][d].wait_send()
            xbs[g][d].wait_send()

        def block(i, carry):
            owner, _, data, scales = zmsg(g, i)

            @pl.when(owner != z)
            def _():
                data.wait_send()
                scales.wait_send()

            return carry

        lax.fori_loop(0, SIZES[g], block, 0)

    def energies():
        for i in range(2, 6):
            loads[i].wait()
        levels = eocc[...].reshape(1, 64)
        tall = jnp.transpose(jnp.broadcast_to(levels, (128, 64)))
        l_id = lax.broadcasted_iota(jnp.int32, (64, BLOCK), 0)
        first, second = occ[0:1, :], occ[1:2, :]
        hot = (jnp.where(l_id == first, 1.0, 0.0) + jnp.where(l_id == second, 1.0, 0.0)).astype(BF16)
        acc = None
        for s in split3(tall):
            term = lax.dot_general(hot, s, (((0,), (0,)), ((), ())), preferred_element_type=F32)
            acc = term if acc is None else acc + term
        up[...] = acc
        e_rows = [jnp.broadcast_to(s.astype(F32), (16, 800)).astype(BF16) for s in split3(evir[...])]

        def tile(t, carry):
            cols = pl.ds(pl.multiple_of(t * 256, 256), 256)
            v_id = lax.broadcasted_iota(jnp.int32, (800, 256), 0)
            a, b = vir[0:1, cols], vir[1:2, cols]
            h = (jnp.where(v_id == a, 1.0, 0.0) + jnp.where(v_id == b, 1.0, 0.0)).astype(BF16)
            v = None
            for s in e_rows:
                term = jnp.dot(s, h, preferred_element_type=F32)
                v = term if v is None else v + term
            vq[:, cols] = v[0:8]
            return carry

        lax.fori_loop(0, NDIM // 256, tile, 0)

    def stored_products():
        loads[6].wait()
        corr_h[...] = jnp.zeros_like(corr_h)

        def tile(t, carry):
            cols = pl.ds(pl.multiple_of(t * 128, 128), 128)
            vals = [err[k, :, cols].astype(F32) for k in range(5)]
            n = 0
            for i in range(5):
                for j in range(i + 1):
                    corr_h[n : n + 1, :] += jnp.sum(vals[i] * vals[j], axis=0, keepdims=True)
                    n += 1
            return carry

        lax.fori_loop(0, NT, tile, 0)

    def send_group(src_ref, dst_ref, k, count, to):
        def one(o, carry):
            remote(src_ref, dst_ref.at[o - 1], c_s.at[k], c_r.at[k], to(o)).start()
            return carry

        lax.fori_loop(1, count, one, 0)

    def wait_group(dst_ref, k):
        remote(dst_ref, dst_ref, c_s.at[k], c_r.at[k], twin).wait_recv()

    def wait_group_sent(dst_ref, k):
        remote(dst_ref, dst_ref, c_s.at[k], c_r.at[k], twin).wait_send()

    def to_col(o):
        return (row, (col + o) % COLS)

    def to_row(o):
        return ((row + o) % ROWS, col)

    def total_of(mine, got):
        return mine[...] + jnp.sum(got[...], axis=0)

    def own_rows(p):
        n = rows_of(p)
        rows = slice(SUB * p, SUB * p + n)
        everything = z_in.at[p]
        remote(everything, everything, z_s.at[0], z_r.at[p], twin).wait_recv()
        scales = zs_in.at[p]
        remote(scales, scales, zs_s.at[0], zs_r.at[p], twin).wait_recv()

        def add(k, total):
            return total + decode(z_in[p, k], zs_in[p, k, 0:1, :])

        ladder = lax.fori_loop(0, NZ - 1, add, z_own[p])[0:n]
        if p == 0:
            loads[7].wait()
            loads[8].wait()
            corr_n[...] = jnp.zeros_like(corr_n)
        gap = widen(up[rows, :], NT) - vq[0:1, :]
        raw = (src[rows, :] + ladder) / gap
        raw_buf[rows, :] = raw
        new = raw - amp[0, rows, :].astype(F32)
        for k in range(5):
            corr_n[k : k + 1, :] += lane_sums(new * err[k, rows, :].astype(F32))
        corr_n[5:6, :] += lane_sums(new * new)

    pl.semaphore_wait(barrier, ROWS + COLS - 2)
    own_up[0].start()
    own_down[0].start()
    for p in range(PIECES):
        own_twin[p].start()
    own_up[1].start()
    own_down[1].start()

    def serve_near(p):
        own_up[p].wait_recv()
        fwd_up[p].start()
        near_twin[0][p].start()
        own_down[p].wait_recv()
        fwd_down[p].start()
        near_twin[1][p].start()
        if p + 2 < PIECES:
            own_up[p + 2].start()
            own_down[p + 2].start()

    def serve_far(p):
        fwd_up[p].wait_recv()
        far_twin[0][p].start()
        fwd_down[p].wait_recv()
        far_twin[1][p].start()

    def arrived(g):
        kind, p = ORDER[g]
        if kind == "own":
            loads[1].wait()
        elif kind == "sib":
            for q in range(PIECES):
                own_twin[q].wait_recv()
        elif kind == "near":
            near_twin[0][p].wait_recv()
            near_twin[1][p].wait_recv()
        else:
            far_twin[0][p].wait_recv()
            far_twin[1][p].wait_recv()

    for g in range(GROUPS):
        kind, p = ORDER[g]
        if kind == "near":
            serve_near(p)
        elif kind == "far":
            serve_far(p)
        arrived(g)
        multiply(g)
        stage_a(g)
        if g >= 1:
            stage_b(g - 1)
        if g >= 2:
            stage_c(g - 2)
        if g == 1:
            stored_products()
            send_group(corr_h, h1_in, 0, COLS, to_col)
        if g == 2:
            energies()
        if g == 4:
            wait_group(h1_in, 0)
            sum_h[...] = total_of(corr_h, h1_in)
            send_group(sum_h, h2_in, 1, ROWS, to_row)
        if g == 7:
            own_rows(0)
        if g == 9:
            own_rows(1)
    stage_b(GROUPS - 1)
    stage_c(GROUPS - 2)
    stage_c(GROUPS - 1)
    own_rows(2)
    own_rows(3)
    send_group(corr_n, n1_in, 2, COLS, to_col)
    for g in range(GROUPS):
        finish_sends(g)
    wait_group(n1_in, 2)
    sum_n[...] = total_of(corr_n, n1_in)
    send_group(sum_n, n2_in, 3, ROWS, to_row)
    for group in [own_up, own_down, own_twin, fwd_up, fwd_down] + near_twin + far_twin:
        for copy in group:
            copy.wait_send()
    wait_group(h2_in, 1)
    stored = jnp.sum(total_of(sum_h, h2_in), axis=1, keepdims=True)
    stored = jnp.broadcast_to(stored, (16, 128))
    for k, ref in enumerate((h1_in, h2_in, n1_in)):
        wait_group_sent(ref, k)
    wait_group(n2_in, 3)
    fresh = jnp.sum(total_of(sum_n, n2_in), axis=1, keepdims=True)
    fresh = jnp.broadcast_to(fresh, (8, 128))
    corr = [[None] * 6 for _ in range(6)]
    n = 0
    for i in range(5):
        for j in range(i + 1):
            corr[i][j] = stored[n : n + 1, :]
            n += 1
    for j in range(6):
        corr[5][j] = fresh[j : j + 1, :]
    weights = [widen(w, NT) for w in solve(corr)]
    for p in range(PIECES):
        rows = slice(SUB * p, SUB * p + rows_of(p))
        total = weights[5] * raw_buf[rows, :]
        for k in range(5):
            total = total + weights[k] * amp[k, rows, :].astype(F32)
        out_ref[rows, :] = total
    wait_group_sent(n2_in, 3)


def on_device(integrals, lambda2, source_terms, hist_amp, hist_err, eps_occ, eps_vir, occ_pair, vir_pair):
    vmem = pltpu.VMEM
    dma = pltpu.SemaphoreType.DMA
    i16 = jnp.int16
    scratch = [
        vmem((KDIM, NDIM), BF16),
        vmem((252, KDIM), BF16),
        vmem((BLOCK, NDIM), F32),
        vmem((5, BLOCK, NDIM), BF16),
        vmem((5, BLOCK, NDIM), BF16),
        vmem((1, 64), F32),
        vmem((1, 800), F32),
        vmem((2, BLOCK), jnp.int32),
        vmem((2, NDIM), jnp.int32),
        vmem((256, KDIM), BF16),
        vmem((256, KDIM), BF16),
        vmem((PIECES, 256, KDIM), BF16),
        vmem((PIECES, 128, KDIM), BF16),
        vmem((GROUPS, 4, NX, SUB, NDIM), F32),
        vmem((GROUPS, 2, 4, SUB, NDIM // 2), i16),
        vmem((GROUPS, 2, 4, SUB, NDIM // 2), i16),
        vmem((GROUPS, 2, 8, 128), F32),
        vmem((GROUPS, 2, 8, 128), F32),
        vmem((GROUPS, 2, 4, SUB, NDIM), i16),
        vmem((GROUPS, 2, 4, SUB, NDIM), i16),
        vmem((GROUPS, 2, 8, 128), F32),
        vmem((GROUPS, 2, 8, 128), F32),
        vmem((ZSENDS, SUB, NDIM), i16),
        vmem((PIECES, NZ - 1, SUB, NDIM), i16),
        vmem((ZSENDS, 8, 128), F32),
        vmem((PIECES, NZ - 1, 8, 128), F32),
        vmem((PIECES, SUB, NDIM), F32),
        vmem((BLOCK, NDIM), F32),
        vmem((BLOCK, 128), F32),
        vmem((8, NDIM), F32),
        vmem((16, 128), F32),
        vmem((8, 128), F32),
        vmem((16, 128), F32),
        vmem((8, 128), F32),
        vmem((COLS - 1, 16, 128), F32),
        vmem((ROWS - 1, 16, 128), F32),
        vmem((COLS - 1, 8, 128), F32),
        vmem((ROWS - 1, 8, 128), F32),
        dma((9,)),
        dma((9 * PIECES,)),
        dma((9 * PIECES,)),
    ] + [dma((GROUPS, 2))] * 8 + [dma((ZSENDS,))] * 2 + [dma((PIECES,))] * 2 + [dma((4,))] * 2
    call = pl.pallas_call(
        kernel,
        out_shape=jax.ShapeDtypeStruct((BLOCK, NDIM), F32),
        in_specs=[pl.BlockSpec(memory_space=pl.ANY)] * 9,
        out_specs=pl.BlockSpec(memory_space=pltpu.VMEM),
        scratch_shapes=scratch,
        compiler_params=pltpu.CompilerParams(
            collective_id=0, has_side_effects=True, vmem_limit_bytes=60 * 1024 * 1024
        ),
        name="ladder",
    )
    return call(
        integrals, lambda2, source_terms, hist_amp, hist_err,
        eps_occ.reshape(1, 64), eps_vir.reshape(1, 800), occ_pair, vir_pair,
    )


def solution(mesh):
    placed = (
        P("row", "col"),
        P("col", "row"),
        P("row", "col"),
        P(None, "row", "col"),
        P(None, "row", "col"),
        P(),
        P(),
        P(None, "row"),
        P(None, "col"),
    )
    return jax.shard_map(
        on_device, mesh=mesh, in_specs=placed, out_specs=P("row", "col"), check_vma=False
    )
```

```python
import functools

import jax
import jax.numpy as jnp
from jax import lax
from jax.experimental import pallas as pl
from jax.experimental.pallas import tpu as pltpu
from jax.sharding import PartitionSpec as P

MESH = pl.DeviceIdType.MESH
F32 = jnp.float32
BF16 = jnp.bfloat16
LEVELS = 32000.0

NX, NY, NZ = 4, 4, 8
ROWS, COLS = NX * NZ, NY * 2
BLOCK = 63
SUB = 16
PIECES = 4
KDIM = 2048
NDIM = 1024
NT = NDIM // 128

GROUP_LIST = [("own", 0, 0, 4), ("sib", 0, 0, 4)]
for _p in range(PIECES):
    GROUP_LIST += [("near", _p, 0, 2), ("near", _p, 2, 2)]
    GROUP_LIST += [("far", _p, 0, 2)] if _p < 3 else [("far", _p, 0, 1), ("far", _p, 1, 1)]
GROUPS = len(GROUP_LIST)
SIZES = tuple(entry[3] for entry in GROUP_LIST)
BASE = tuple(sum(SIZES[:g]) for g in range(GROUPS))
UNITS = sum(SIZES)

SEQUENCE = (
    "m0", "k0", "m1", "k1", "b0", "h0", "s0", "b1", "m2", "m3", "c0", "e0", "s1", "m5", "b2", "c1",
    "b3", "m6", "f0", "b5", "m4", "c2", "h1", "c3", "b6", "s2", "m8", "c5", "b4", "m9", "f1", "c6",
    "b8", "m7", "c4", "b9", "c8", "b7", "s3", "m11", "c9", "m12", "f2", "c7", "b11", "m10", "d0",
    "h2", "b12", "f3", "m13", "m14", "c11", "b10", "c12", "b13", "d1", "b14", "c10", "c13", "c14",
    "d2", "d3",
)


def rows_of(piece):
    return SUB if piece < PIECES - 1 else BLOCK - SUB * (PIECES - 1)


def widen(row, count):
    return jnp.concatenate([row] * count, axis=1)


def fold(values, op):
    out = values[:, 0:128]
    for j in range(1, values.shape[1] // 128):
        out = op(out, values[:, 128 * j : 128 * (j + 1)])
    return out


def encode(values):
    top = jnp.max(fold(jnp.abs(values), jnp.maximum), axis=0, keepdims=True)
    top = jnp.maximum(top, 1e-30)
    factor = widen(LEVELS / top, values.shape[1] // 128)
    code = jnp.round(values * factor).astype(jnp.int32).astype(jnp.int16)
    return code, top * (1.0 / LEVELS)


def decode(code, scale):
    return code.astype(jnp.int32).astype(F32) * widen(scale, code.shape[1] // 128)


def split3(values):
    high = values.astype(BF16)
    rest = values - high.astype(F32)
    middle = rest.astype(BF16)
    low = (rest - middle.astype(F32)).astype(BF16)
    return high, middle, low


def lane_sums(values):
    return jnp.sum(fold(values, jnp.add), axis=0, keepdims=True)


def solve(corr):
    factor = [[None] * 6 for _ in range(6)]
    for j in range(6):
        for i in range(j, 6):
            run = corr[i][j]
            for k in range(j):
                run = run - factor[i][k] * factor[j][k]
            if i == j:
                factor[j][j] = jnp.sqrt(run)
            else:
                factor[i][j] = run / factor[j][j]
    forward = []
    for k in range(6):
        run = jnp.ones_like(corr[0][0])
        for m in range(k):
            run = run - factor[k][m] * forward[m]
        forward.append(run / factor[k][k])
    back = [None] * 6
    for k in reversed(range(6)):
        run = forward[k]
        for m in range(k + 1, 6):
            run = run - factor[m][k] * back[m]
        back[k] = run / factor[k][k]
    total = back[0]
    for k in range(1, 6):
        total = total + back[k]
    return [b / total for b in back]


def kernel(
    ints_hbm, lam_hbm, src_hbm, amp_hbm, err_hbm, eocc_hbm, evir_hbm, occ_hbm, vir_hbm,
    out_ref,
    ints, lam, src, amp, err, eocc, evir, occ, vir,
    a_own, a_sib, a_near, a_far, part,
    xa_out, xa_in, xas_out, xas_in, xb_out, xb_in, xbs_out, xbs_in,
    z_out, z_in, zs_out, zs_in, z_own,
    raw_buf, up, vq, corr_h, corr_n, sums, h1_in, h2_in, n1_in, n2_in,
    greet, load_sem, ag_send, ag_recv, xa_s, xa_r, xas_s, xas_r, xb_s, xb_r, xbs_s, xbs_r,
    z_s, zs_s, z_r, zs_r, c_s, c_r,
):
    row = lax.axis_index("row")
    col = lax.axis_index("col")
    z, x = row // NX, row % NX
    y, core = col // 2, col % 2
    sib = 1 - core
    xp, xm, xo = (x + 1) % NX, (x + 3) % NX, (x + 2) % NX
    yp, ym = (y + 1) % NY, (y + 3) % NY

    def at_y(yy):
        return (row, yy * 2 + core)

    def at_x(xx):
        return (z * NX + xx, col)

    twin = (row, y * 2 + sib)

    barrier = pltpu.get_barrier_semaphore()
    zp, zm = (z + 1) % NZ, (z + 7) % NZ
    direct = [twin, at_y(yp), at_y(ym), at_x(xp), at_x(xm), (zp * NX + x, col), (zm * NX + x, col)]
    for dev in direct:
        pl.semaphore_signal(barrier, inc=1, device_id=dev, device_id_type=MESH)

    loads = [
        pltpu.make_async_copy(s, d, load_sem.at[i])
        for i, (s, d) in enumerate(
            (
                (lam_hbm, lam), (ints_hbm, ints), (eocc_hbm, eocc), (evir_hbm, evir),
                (occ_hbm, occ), (vir_hbm, vir), (err_hbm, err), (src_hbm, src), (amp_hbm, amp),
            )
        )
    ]
    loads[0].start()

    loads[0].wait()
    for load in loads[1:]:
        load.start()
    r_id = lax.broadcasted_iota(jnp.int32, (256, 252), 0)
    s_id = lax.broadcasted_iota(jnp.int32, (256, 252), 1)
    inner = (r_id // 64) * SUB + r_id % SUB
    source = ((r_id % 64) // SUB) * BLOCK + inner
    pick = jnp.where((source == s_id) & (inner < BLOCK), 1.0, 0.0).astype(BF16)

    def permute(t, carry):
        cols = pl.ds(pl.multiple_of(t * 512, 512), 512)
        a_own[:, cols] = jnp.dot(pick, lam[:, cols], preferred_element_type=F32).astype(BF16)
        return carry

    lax.fori_loop(0, KDIM // 512, permute, 0)

    def remote(src_ref, dst_ref, ssem, rsem, dev):
        return pltpu.make_async_remote_copy(
            src_ref=src_ref, dst_ref=dst_ref, send_sem=ssem, recv_sem=rsem,
            device_id=dev, device_id_type=MESH,
        )

    def ag(kind, p, s, d, dev):
        k = kind * PIECES + p
        return remote(s, d, ag_send.at[k], ag_recv.at[k], dev)

    def piece_of(ref, p):
        return ref.at[pl.ds(64 * p, 64)]

    def near(p, slot):
        return a_near.at[p, pl.ds(64 * slot, 64)]

    def far(p, slot, half):
        return a_far.at[p, pl.ds(64 * slot + 32 * half, 32)]

    own_up = [ag(0, p, piece_of(a_own, p), near(p, 0), at_y(yp)) for p in range(PIECES)]
    own_down = [ag(1, p, piece_of(a_own, p), near(p, 1), at_y(ym)) for p in range(PIECES)]
    own_twin = [ag(2, p, piece_of(a_own, p), piece_of(a_sib, p), twin) for p in range(PIECES)]
    fwd_up = [
        ag(3, p, a_near.at[p, pl.ds(0, 32)], far(p, 0, 0), at_y(yp)) for p in range(PIECES)
    ]
    fwd_down = [
        ag(4, p, a_near.at[p, pl.ds(96, 32)], far(p, 0, 1), at_y(ym)) for p in range(PIECES)
    ]
    near_twin = [
        [ag(5 + s, p, near(p, s), near(p, 2 + s), twin) for p in range(PIECES)] for s in range(2)
    ]
    far_twin = [
        [ag(7 + h, p, far(p, 0, h), far(p, 1, h), twin) for p in range(PIECES)] for h in range(2)
    ]

    def multiply(g):
        kind, p, first, n = GROUP_LIST[g]
        rows = pl.ds(64 * first, 64 * n)
        a = {"own": a_own, "sib": a_sib}.get(kind)
        if a is None:
            a = (a_near if kind == "near" else a_far).at[p, rows]

        def tile(t, carry):
            cols = pl.ds(pl.multiple_of(t * 1024, 1024), 1024)
            res = jnp.dot(a[...], ints[:, cols], preferred_element_type=F32)
            part[BASE[g] : BASE[g] + n, :, :, cols] = res.reshape(n, NX, SUB, 1024)
            return carry

        lax.fori_loop(0, NDIM // 1024, tile, 0)

    def xmsg(out, inn, ss, rs, g, d, dev):
        units = pl.ds(BASE[g], SIZES[g])
        return remote(out.at[d, units], inn.at[d, units], ss.at[g, d], rs.at[g, d], dev)

    sides = (xp, xm)

    def xmsgs(out, inn, ss, rs):
        return [[xmsg(out, inn, ss, rs, g, d, at_x(sides[d])) for d in range(2)] for g in range(GROUPS)]

    xa = xmsgs(xa_out, xa_in, xa_s, xa_r)
    xas = xmsgs(xas_out, xas_in, xas_s, xas_r)
    xb = xmsgs(xb_out, xb_in, xb_s, xb_r)
    xbs = xmsgs(xbs_out, xbs_in, xbs_s, xbs_r)

    def units_of(g, body):
        lax.fori_loop(BASE[g], BASE[g] + SIZES[g], lambda k, carry: body(k) or carry, 0)

    def stage_a(g):
        def block(k):
            for d in range(2):
                code, scale = encode(part[k, xo, :, 512 * d : 512 * (d + 1)])
                xa_out[d, k] = code
                xas_out[d, k] = scale

        units_of(g, block)
        for d in range(2):
            xa[g][d].start()
            xas[g][d].start()

    def stage_b(g):
        for d in range(2):
            xa[g][d].wait_recv()
            xas[g][d].wait_recv()

        def block(k):
            for d in range(2):
                mine = part[k, sides[d]]
                got = decode(xa_in[d, k], xas_in[d, k])
                if d == 0:
                    both = jnp.concatenate([mine[:, :512] + got, mine[:, 512:]], axis=1)
                else:
                    both = jnp.concatenate([mine[:, :512], mine[:, 512:] + got], axis=1)
                code, scale = encode(both)
                xb_out[d, k] = code
                xbs_out[d, k] = scale

        units_of(g, block)
        for d in range(2):
            xb[g][d].start()
            xbs[g][d].start()

    def place(g, k):
        kind, p, first, _ = GROUP_LIST[g]
        i = k - BASE[g] + first
        if kind == "own":
            return col, i
        if kind == "sib":
            return y * 2 + sib, i
        if kind == "near":
            return ((y + 3 + 2 * (i % 2)) % NY) * 2 + (core + i // 2) % 2, p
        return ((y + 2) % NY) * 2 + (core + i) % 2, p

    def zmsg(g, k):
        owner, p = place(g, k)
        slot = (z - owner + NZ - 1) % NZ
        dev = (owner * NX + x, col)
        return (
            owner,
            p,
            remote(z_out.at[k], z_in.at[p, slot], z_s.at[k], z_r.at[p], dev),
            remote(zs_out.at[k], zs_in.at[p, slot], zs_s.at[k], zs_r.at[p], dev),
        )

    def stage_c(g):
        for d in range(2):
            xb[g][d].wait_recv()
            xbs[g][d].wait_recv()

        def block(k):
            owner, p, data, scales = zmsg(g, k)
            total = part[k, x]
            for d in range(2):
                total = total + decode(xb_in[d, k], xbs_in[d, k])

            @pl.when(owner == z)
            def _():
                z_own[p] = total

            @pl.when(owner != z)
            def _():
                code, scale = encode(total)
                z_out[k] = code
                zs_out[k] = scale
                data.start()
                scales.start()

        units_of(g, block)

    def finish_sends(g):
        for d in range(2):
            xa[g][d].wait_send()
            xas[g][d].wait_send()
            xb[g][d].wait_send()
            xbs[g][d].wait_send()

        def block(k):
            owner, _, data, scales = zmsg(g, k)

            @pl.when(owner != z)
            def _():
                data.wait_send()
                scales.wait_send()

        units_of(g, block)

    def energies():
        for i in range(2, 6):
            loads[i].wait()
        levels = eocc[...].reshape(1, 64)
        tall = jnp.transpose(jnp.broadcast_to(levels, (128, 64)))
        l_id = lax.broadcasted_iota(jnp.int32, (64, BLOCK), 0)
        first, second = occ[0:1, :], occ[1:2, :]
        hot = (jnp.where(l_id == first, 1.0, 0.0) + jnp.where(l_id == second, 1.0, 0.0)).astype(BF16)
        acc = None
        for s in split3(tall):
            term = lax.dot_general(hot, s, (((0,), (0,)), ((), ())), preferred_element_type=F32)
            acc = term if acc is None else acc + term
        up[...] = acc
        e_rows = [jnp.broadcast_to(s.astype(F32), (16, 800)).astype(BF16) for s in split3(evir[...].reshape(1, 800))]

        def tile(t, carry):
            cols = pl.ds(pl.multiple_of(t * 256, 256), 256)
            v_id = lax.broadcasted_iota(jnp.int32, (800, 256), 0)
            a, b = vir[0:1, cols], vir[1:2, cols]
            h = (jnp.where(v_id == a, 1.0, 0.0) + jnp.where(v_id == b, 1.0, 0.0)).astype(BF16)
            v = None
            for s in e_rows:
                term = jnp.dot(s, h, preferred_element_type=F32)
                v = term if v is None else v + term
            vq[:, cols] = v[0:8]
            return carry

        lax.fori_loop(0, NDIM // 256, tile, 0)

    def stored_products():
        loads[6].wait()
        corr_h[...] = jnp.zeros_like(corr_h)

        def tile(t, carry):
            cols = pl.ds(pl.multiple_of(t * 128, 128), 128)
            vals = [err[k, :, cols].astype(F32) for k in range(5)]
            n = 0
            for i in range(5):
                for j in range(i + 1):
                    corr_h[n : n + 1, :] += jnp.sum(vals[i] * vals[j], axis=0, keepdims=True)
                    n += 1
            return carry

        lax.fori_loop(0, NT, tile, 0)

    def send_group(src_ref, dst_ref, k, count, to):
        def one(o, carry):
            remote(src_ref, dst_ref.at[o - 1], c_s.at[k], c_r.at[k], to(o)).start()
            return carry

        lax.fori_loop(1, count, one, 0)

    def wait_group(dst_ref, k):
        remote(dst_ref, dst_ref, c_s.at[k], c_r.at[k], twin).wait_recv()

    def wait_group_sent(dst_ref, k):
        remote(dst_ref, dst_ref, c_s.at[k], c_r.at[k], twin).wait_send()

    def to_col(o):
        return (row, (col + o) % COLS)

    def to_row(o):
        return ((row + o) % ROWS, col)

    def total_of(k, got):
        return sums[k] + jnp.sum(got[...], axis=0)

    eye = lax.broadcasted_iota(jnp.int32, (16, 128), 0) == lax.broadcasted_iota(jnp.int32, (16, 128), 1)

    def pack(values):
        tall = jnp.broadcast_to(jnp.sum(values, axis=1, keepdims=True), (16, 128))
        return jnp.sum(jnp.where(eye, tall, 0.0), axis=0, keepdims=True)

    def unpack(values):
        tall = jnp.where(eye, jnp.broadcast_to(values, (16, 128)), 0.0)
        return jnp.broadcast_to(jnp.sum(tall, axis=1, keepdims=True), (16, 128))

    def own_rows(p):
        n = rows_of(p)
        rows = slice(SUB * p, SUB * p + n)
        everything = z_in.at[p]
        remote(everything, everything, z_s.at[0], z_r.at[p], twin).wait_recv()
        scales = zs_in.at[p]
        remote(scales, scales, zs_s.at[0], zs_r.at[p], twin).wait_recv()

        def add(k, total):
            return total + decode(z_in[p, k], zs_in[p, k])

        ladder = lax.fori_loop(0, NZ - 1, add, z_own[p])[0:n]
        if p == 0:
            loads[7].wait()
            loads[8].wait()
            corr_n[...] = jnp.zeros_like(corr_n)
        gap = widen(up[rows, :], NT) - vq[0:1, :]
        raw = (src[rows, :] + ladder) / gap
        raw_buf[rows, :] = raw
        new = raw - amp[0, rows, :].astype(F32)
        for k in range(5):
            corr_n[k : k + 1, :] += lane_sums(new * err[k, rows, :].astype(F32))
        corr_n[5:6, :] += lane_sums(new * new)

    def greet_z(i):
        for far_z in ((z + 1 + i) % NZ, (z + NZ - 1 - i) % NZ):
            pl.semaphore_signal(greet.at[i], inc=1, device_id=(far_z * NX + x, col), device_id_type=MESH)

    pl.semaphore_wait(barrier, len(direct))
    greet_z(0)
    own_up[0].start()
    own_down[0].start()
    for p in range(PIECES):
        own_twin[p].start()
    own_up[1].start()
    own_down[1].start()

    def serve_near(p):
        own_up[p].wait_recv()
        fwd_up[p].start()
        near_twin[0][p].start()
        own_down[p].wait_recv()
        fwd_down[p].start()
        near_twin[1][p].start()
        if p + 2 < PIECES:
            own_up[p + 2].start()
            own_down[p + 2].start()

    def serve_far(p):
        fwd_up[p].wait_recv()
        far_twin[0][p].start()
        fwd_down[p].wait_recv()
        far_twin[1][p].start()

    def arrived(g):
        kind, p, first, n = GROUP_LIST[g]
        if kind == "own":
            loads[1].wait()
        elif kind == "sib":
            for q in range(PIECES):
                own_twin[q].wait_recv()
        elif kind == "near" and first + n == 4:
            near_twin[0][p].wait_recv()
            near_twin[1][p].wait_recv()
        elif kind == "far" and first + n == 2:
            far_twin[0][p].wait_recv()
            far_twin[1][p].wait_recv()

    def run_multiply(g):
        arrived(g)
        multiply(g)
        stage_a(g)

    def greetings(i):
        pl.semaphore_wait(greet.at[i], 2)
        if i == 0:
            greet_z(1)

    def products(i):
        if i == 0:
            stored_products()
            sums[0] = pack(corr_h[...])
        elif i == 1:
            send_group(sums.at[0], h1_in, 0, COLS, to_col)
        else:
            wait_group(h1_in, 0)
            sums[1] = total_of(0, h1_in)
            send_group(sums.at[1], h2_in, 1, ROWS, to_row)

    steps = {
        "m": run_multiply, "b": stage_b, "c": stage_c, "d": own_rows, "s": serve_near,
        "f": serve_far, "k": greetings, "h": products, "e": lambda i: energies(),
    }
    for step in SEQUENCE:
        steps[step[0]](int(step[1:]))
    sums[2] = pack(corr_n[...])
    send_group(sums.at[2], n1_in, 2, COLS, to_col)
    for g in range(GROUPS):
        finish_sends(g)
    wait_group(n1_in, 2)
    sums[3] = total_of(2, n1_in)
    send_group(sums.at[3], n2_in, 3, ROWS, to_row)
    for group in [own_up, own_down, own_twin, fwd_up, fwd_down] + near_twin + far_twin:
        for copy in group:
            copy.wait_send()
    wait_group(h2_in, 1)
    stored = unpack(total_of(1, h2_in))
    for k, ref in enumerate((h1_in, h2_in, n1_in)):
        wait_group_sent(ref, k)
    wait_group(n2_in, 3)
    fresh = unpack(total_of(3, n2_in))
    corr = [[None] * 6 for _ in range(6)]
    n = 0
    for i in range(5):
        for j in range(i + 1):
            corr[i][j] = stored[n : n + 1, :]
            n += 1
    for j in range(6):
        corr[5][j] = fresh[j : j + 1, :]
    weights = [widen(w, NT) for w in solve(corr)]
    for p in range(PIECES):
        rows = slice(SUB * p, SUB * p + rows_of(p))
        total = weights[5] * raw_buf[rows, :]
        for k in range(5):
            total = total + weights[k] * amp[k, rows, :].astype(F32)
        out_ref[rows, :] = total
    wait_group_sent(n2_in, 3)


def on_device(integrals, lambda2, source_terms, hist_amp, hist_err, eps_occ, eps_vir, occ_pair, vir_pair):
    vmem = pltpu.VMEM
    dma = pltpu.SemaphoreType.DMA
    i16 = jnp.int16
    scratch = [
        vmem((KDIM, NDIM), BF16),
        vmem((252, KDIM), BF16),
        vmem((BLOCK, NDIM), F32),
        vmem((5, BLOCK, NDIM), BF16),
        vmem((5, BLOCK, NDIM), BF16),
        vmem((1, 64), F32),
        vmem((800,), F32),
        vmem((2, BLOCK), jnp.int32),
        vmem((2, NDIM), jnp.int32),
        vmem((256, KDIM), BF16),
        vmem((256, KDIM), BF16),
        vmem((PIECES, 256, KDIM), BF16),
        vmem((PIECES, 128, KDIM), BF16),
        vmem((UNITS, NX, SUB, NDIM), F32),
        vmem((2, UNITS, SUB, NDIM // 2), i16),
        vmem((2, UNITS, SUB, NDIM // 2), i16),
        vmem((2, UNITS, 1, 128), F32),
        vmem((2, UNITS, 1, 128), F32),
        vmem((2, UNITS, SUB, NDIM), i16),
        vmem((2, UNITS, SUB, NDIM), i16),
        vmem((2, UNITS, 1, 128), F32),
        vmem((2, UNITS, 1, 128), F32),
        vmem((UNITS, SUB, NDIM), i16),
        vmem((PIECES, NZ - 1, SUB, NDIM), i16),
        vmem((UNITS, 1, 128), F32),
        vmem((PIECES, NZ - 1, 1, 128), F32),
        vmem((PIECES, SUB, NDIM), F32),
        vmem((BLOCK, NDIM), F32),
        vmem((BLOCK, 128), F32),
        vmem((8, NDIM), F32),
        vmem((16, 128), F32),
        vmem((16, 128), F32),
        vmem((4, 1, 128), F32),
        vmem((COLS - 1, 1, 128), F32),
        vmem((ROWS - 1, 1, 128), F32),
        vmem((COLS - 1, 1, 128), F32),
        vmem((ROWS - 1, 1, 128), F32),
        pltpu.SemaphoreType.REGULAR((2,)),
        dma((9,)),
        dma((9 * PIECES,)),
        dma((9 * PIECES,)),
    ] + [dma((GROUPS, 2))] * 8 + [dma((UNITS,))] * 2 + [dma((PIECES,))] * 2 + [dma((4,))] * 2
    call = pl.pallas_call(
        kernel,
        out_shape=jax.ShapeDtypeStruct((BLOCK, NDIM), F32),
        in_specs=[pl.BlockSpec(memory_space=pltpu.HBM)] * 9,
        out_specs=pl.BlockSpec(memory_space=pltpu.VMEM),
        scratch_shapes=scratch,
        compiler_params=pltpu.CompilerParams(
            collective_id=0, has_side_effects=True, vmem_limit_bytes=44 * 1024 * 1024
        ),
        name="ladder",
    )
    operands = (
        integrals, lambda2, source_terms, hist_amp, hist_err,
        eps_occ.reshape(1, 64), eps_vir, occ_pair, vir_pair,
    )
    return call(*[pltpu.with_memory_space_constraint(o, pltpu.HBM) for o in operands])


def solution(mesh):
    placed = (
        P("row", "col"),
        P("col", "row"),
        P("row", "col"),
        P(None, "row", "col"),
        P(None, "row", "col"),
        P(),
        P(),
        P(None, "row"),
        P(None, "col"),
    )
    return jax.shard_map(
        on_device, mesh=mesh, in_specs=placed, out_specs=P("row", "col"), check_vma=False
    )
```

```python
import functools

import jax
import jax.numpy as jnp
from jax import lax
from jax.experimental import pallas as pl
from jax.experimental.pallas import tpu as pltpu
from jax.sharding import PartitionSpec as P

MESH = pl.DeviceIdType.MESH
F32 = jnp.float32
BF16 = jnp.bfloat16
LEVELS = 32000.0

NX, NY, NZ = 4, 4, 8
ROWS, COLS = NX * NZ, NY * 2
BLOCK = 63
SUB = 16
PIECES = 4
LEAD = 2
KDIM = 2048
NDIM = 1024
NT = NDIM // 128

GROUP_LIST = [
    ("own", 0, 0, 4), ("sib", 0, 0, 4), ("near", 0, 0, 2), ("near", 0, 2, 2),
    ("far", 0, 0, 2), ("near", 1, 0, 2), ("near", 1, 2, 2), ("far", 1, 0, 2),
    ("near", 2, 0, 2), ("near", 2, 2, 2), ("far", 2, 0, 2), ("near", 3, 0, 2),
    ("near", 3, 2, 2), ("far", 3, 0, 1), ("far", 3, 1, 1),
]
GROUPS = len(GROUP_LIST)
SIZES = tuple(entry[3] for entry in GROUP_LIST)
BASE = tuple(sum(SIZES[:g]) for g in range(GROUPS))
UNITS = sum(SIZES)

SEQUENCE = (
    "m0", "k0", "m1", "k1", "b0", "h0", "b1", "s0", "m2", "m3", "s1", "m5", "b2", "c1", "e0", "f0",
    "m4", "h1", "b3", "b5", "m6", "c2", "s2", "b4", "m8", "c3", "m9", "f1", "c0", "b6", "c5", "m7",
    "b8", "c4", "b9", "s3", "m11", "b7", "c8", "c6", "m12", "f2", "c9", "b11", "m10", "f3", "b12",
    "c7", "m13", "m14", "b10", "c11", "c12", "b13", "b14", "c10", "c13", "c14", "d0", "h2", "d1",
    "d2", "d3",
)


def rows_of(piece):
    return SUB if piece < PIECES - 1 else BLOCK - SUB * (PIECES - 1)


def widen(row, count):
    return jnp.concatenate([row] * count, axis=1)


def fold(values, op):
    out = values[:, 0:128]
    for j in range(1, values.shape[1] // 128):
        out = op(out, values[:, 128 * j : 128 * (j + 1)])
    return out


def encode(values):
    top = jnp.max(fold(jnp.abs(values), jnp.maximum), axis=0, keepdims=True)
    top = jnp.maximum(top, 1e-30)
    factor = widen(LEVELS / top, values.shape[1] // 128)
    code = jnp.round(values * factor).astype(jnp.int32).astype(jnp.int16)
    return code, top * (1.0 / LEVELS)


def decode(code, scale):
    return code.astype(jnp.int32).astype(F32) * widen(scale, code.shape[1] // 128)


def split3(values):
    high = values.astype(BF16)
    rest = values - high.astype(F32)
    middle = rest.astype(BF16)
    low = (rest - middle.astype(F32)).astype(BF16)
    return high, middle, low


def lane_sums(values):
    return jnp.sum(fold(values, jnp.add), axis=0, keepdims=True)


def solve(corr):
    factor = [[None] * 6 for _ in range(6)]
    for j in range(6):
        for i in range(j, 6):
            run = corr[i][j]
            for k in range(j):
                run = run - factor[i][k] * factor[j][k]
            if i == j:
                factor[j][j] = jnp.sqrt(run)
            else:
                factor[i][j] = run / factor[j][j]
    forward = []
    for k in range(6):
        run = jnp.ones_like(corr[0][0])
        for m in range(k):
            run = run - factor[k][m] * forward[m]
        forward.append(run / factor[k][k])
    back = [None] * 6
    for k in reversed(range(6)):
        run = forward[k]
        for m in range(k + 1, 6):
            run = run - factor[m][k] * back[m]
        back[k] = run / factor[k][k]
    total = back[0]
    for k in range(1, 6):
        total = total + back[k]
    return [b / total for b in back]


def kernel(
    ints_hbm, lam_hbm, src_hbm, amp_hbm, err_hbm, eocc_hbm, evir_hbm, occ_hbm, vir_hbm,
    out_ref,
    ints, lam, src, amp, err, eocc, evir, occ, vir,
    a_own, a_sib, a_near, a_far, part,
    xa_out, xa_in, xas_out, xas_in, xb_out, xb_in, xbs_out, xbs_in,
    z_out, z_in, zs_out, zs_in, z_own,
    raw_buf, up, vq, corr_h, corr_n, sums, h1_in, h2_in, n1_in, n2_in,
    greet, load_sem, ag_send, ag_recv, xa_s, xa_r, xas_s, xas_r, xb_s, xb_r, xbs_s, xbs_r,
    z_s, zs_s, z_r, zs_r, c_s, c_r,
):
    row = lax.axis_index("row")
    col = lax.axis_index("col")
    z, x = row // NX, row % NX
    y, core = col // 2, col % 2
    sib = 1 - core
    xp, xm, xo = (x + 1) % NX, (x + 3) % NX, (x + 2) % NX
    yp, ym = (y + 1) % NY, (y + 3) % NY

    def at_y(yy):
        return (row, yy * 2 + core)

    def at_x(xx):
        return (z * NX + xx, col)

    twin = (row, y * 2 + sib)

    barrier = pltpu.get_barrier_semaphore()
    zp, zm = (z + 1) % NZ, (z + 7) % NZ
    direct = [twin, at_y(yp), at_y(ym), at_x(xp), at_x(xm), (zp * NX + x, col), (zm * NX + x, col)]
    for dev in direct:
        pl.semaphore_signal(barrier, inc=1, device_id=dev, device_id_type=MESH)

    loads = [
        pltpu.make_async_copy(s, d, load_sem.at[i])
        for i, (s, d) in enumerate(
            (
                (lam_hbm, lam), (ints_hbm, ints), (eocc_hbm, eocc), (evir_hbm, evir),
                (occ_hbm, occ), (vir_hbm, vir), (err_hbm, err), (src_hbm, src), (amp_hbm, amp),
            )
        )
    ]
    loads[0].start()

    loads[0].wait()
    for load in loads[1:]:
        load.start()
    r_id = lax.broadcasted_iota(jnp.int32, (256, 252), 0)
    s_id = lax.broadcasted_iota(jnp.int32, (256, 252), 1)
    inner = (r_id // 64) * SUB + r_id % SUB
    source = ((r_id % 64) // SUB) * BLOCK + inner
    pick = jnp.where((source == s_id) & (inner < BLOCK), 1.0, 0.0).astype(BF16)

    def permute(t, carry):
        cols = pl.ds(pl.multiple_of(t * 512, 512), 512)
        a_own[:, cols] = jnp.dot(pick, lam[:, cols], preferred_element_type=F32).astype(BF16)
        return carry

    lax.fori_loop(0, KDIM // 512, permute, 0)

    def remote(src_ref, dst_ref, ssem, rsem, dev):
        return pltpu.make_async_remote_copy(
            src_ref=src_ref, dst_ref=dst_ref, send_sem=ssem, recv_sem=rsem,
            device_id=dev, device_id_type=MESH,
        )

    def ag(kind, p, s, d, dev):
        k = kind * PIECES + p
        return remote(s, d, ag_send.at[k], ag_recv.at[k], dev)

    def piece_of(ref, p):
        return ref.at[pl.ds(64 * p, 64)]

    def near(p, slot):
        return a_near.at[p, pl.ds(64 * slot, 64)]

    def far(p, slot, half):
        return a_far.at[p, pl.ds(64 * slot + 32 * half, 32)]

    own_up = [ag(0, p, piece_of(a_own, p), near(p, 0), at_y(yp)) for p in range(PIECES)]
    own_down = [ag(1, p, piece_of(a_own, p), near(p, 1), at_y(ym)) for p in range(PIECES)]
    own_twin = [ag(2, p, piece_of(a_own, p), piece_of(a_sib, p), twin) for p in range(PIECES)]
    fwd_up = [
        ag(3, p, a_near.at[p, pl.ds(0, 32)], far(p, 0, 0), at_y(yp)) for p in range(PIECES)
    ]
    fwd_down = [
        ag(4, p, a_near.at[p, pl.ds(96, 32)], far(p, 0, 1), at_y(ym)) for p in range(PIECES)
    ]
    near_twin = [
        [ag(5 + s, p, near(p, s), near(p, 2 + s), twin) for p in range(PIECES)] for s in range(2)
    ]
    far_twin = [
        [ag(7 + h, p, far(p, 0, h), far(p, 1, h), twin) for p in range(PIECES)] for h in range(2)
    ]

    def multiply(g):
        kind, p, first, n = GROUP_LIST[g]
        rows = pl.ds(64 * first, 64 * n)
        a = {"own": a_own, "sib": a_sib}.get(kind)
        if a is None:
            a = (a_near if kind == "near" else a_far).at[p, rows]

        def tile(t, carry):
            cols = pl.ds(pl.multiple_of(t * 1024, 1024), 1024)
            res = jnp.dot(a[...], ints[:, cols], preferred_element_type=F32)
            part[BASE[g] : BASE[g] + n, :, :, cols] = res.reshape(n, NX, SUB, 1024)
            return carry

        lax.fori_loop(0, NDIM // 1024, tile, 0)

    def xmsg(out, inn, ss, rs, g, d, dev):
        units = pl.ds(BASE[g], SIZES[g])
        return remote(out.at[d, units], inn.at[d, units], ss.at[g, d], rs.at[g, d], dev)

    sides = (xp, xm)

    def xmsgs(out, inn, ss, rs):
        return [[xmsg(out, inn, ss, rs, g, d, at_x(sides[d])) for d in range(2)] for g in range(GROUPS)]

    xa = xmsgs(xa_out, xa_in, xa_s, xa_r)
    xas = xmsgs(xas_out, xas_in, xas_s, xas_r)
    xb = xmsgs(xb_out, xb_in, xb_s, xb_r)
    xbs = xmsgs(xbs_out, xbs_in, xbs_s, xbs_r)

    def units_of(g, body):
        lax.fori_loop(BASE[g], BASE[g] + SIZES[g], lambda k, carry: body(k) or carry, 0)

    def stage_a(g):
        def block(k):
            for d in range(2):
                code, scale = encode(part[k, xo, :, 512 * d : 512 * (d + 1)])
                xa_out[d, k] = code
                xas_out[d, k] = scale

        units_of(g, block)
        for d in range(2):
            xa[g][d].start()
            xas[g][d].start()

    def stage_b(g):
        for d in range(2):
            xa[g][d].wait_recv()
            xas[g][d].wait_recv()

        def block(k):
            for d in range(2):
                mine = part[k, sides[d]]
                got = decode(xa_in[d, k], xas_in[d, k])
                if d == 0:
                    both = jnp.concatenate([mine[:, :512] + got, mine[:, 512:]], axis=1)
                else:
                    both = jnp.concatenate([mine[:, :512], mine[:, 512:] + got], axis=1)
                code, scale = encode(both)
                xb_out[d, k] = code
                xbs_out[d, k] = scale

        units_of(g, block)
        for d in range(2):
            xb[g][d].start()
            xbs[g][d].start()

    def place(g, k):
        kind, p, first, _ = GROUP_LIST[g]
        i = k - BASE[g] + first
        if kind == "own":
            return col, i
        if kind == "sib":
            return y * 2 + sib, i
        if kind == "near":
            return ((y + 3 + 2 * (i % 2)) % NY) * 2 + (core + i // 2) % 2, p
        return ((y + 2) % NY) * 2 + (core + i) % 2, p

    def zmsg(g, k):
        owner, p = place(g, k)
        slot = (z - owner + NZ - 1) % NZ
        dev = (owner * NX + x, col)
        return (
            owner,
            p,
            remote(z_out.at[k], z_in.at[p, slot], z_s.at[k], z_r.at[p], dev),
            remote(zs_out.at[k], zs_in.at[p, slot], zs_s.at[k], zs_r.at[p], dev),
        )

    def stage_c(g):
        for d in range(2):
            xb[g][d].wait_recv()
            xbs[g][d].wait_recv()

        def block(k):
            owner, p, data, scales = zmsg(g, k)
            total = part[k, x]
            for d in range(2):
                total = total + decode(xb_in[d, k], xbs_in[d, k])

            @pl.when(owner == z)
            def _():
                z_own[p] = total

            @pl.when(owner != z)
            def _():
                code, scale = encode(total)
                z_out[k] = code
                zs_out[k] = scale
                data.start()
                scales.start()

        units_of(g, block)

    def finish_sends(g):
        for d in range(2):
            xa[g][d].wait_send()
            xas[g][d].wait_send()
            xb[g][d].wait_send()
            xbs[g][d].wait_send()

        def block(k):
            owner, _, data, scales = zmsg(g, k)

            @pl.when(owner != z)
            def _():
                data.wait_send()
                scales.wait_send()

        units_of(g, block)

    def energies():
        for i in range(2, 6):
            loads[i].wait()
        levels = eocc[...].reshape(1, 64)
        tall = jnp.transpose(jnp.broadcast_to(levels, (128, 64)))
        l_id = lax.broadcasted_iota(jnp.int32, (64, BLOCK), 0)
        first, second = occ[0:1, :], occ[1:2, :]
        hot = (jnp.where(l_id == first, 1.0, 0.0) + jnp.where(l_id == second, 1.0, 0.0)).astype(BF16)
        acc = None
        for s in split3(tall):
            term = lax.dot_general(hot, s, (((0,), (0,)), ((), ())), preferred_element_type=F32)
            acc = term if acc is None else acc + term
        up[...] = acc
        e_rows = [jnp.broadcast_to(s.astype(F32), (16, 800)).astype(BF16) for s in split3(evir[...].reshape(1, 800))]

        def tile(t, carry):
            cols = pl.ds(pl.multiple_of(t * 256, 256), 256)
            v_id = lax.broadcasted_iota(jnp.int32, (800, 256), 0)
            a, b = vir[0:1, cols], vir[1:2, cols]
            h = (jnp.where(v_id == a, 1.0, 0.0) + jnp.where(v_id == b, 1.0, 0.0)).astype(BF16)
            v = None
            for s in e_rows:
                term = jnp.dot(s, h, preferred_element_type=F32)
                v = term if v is None else v + term
            vq[:, cols] = v[0:8]
            return carry

        lax.fori_loop(0, NDIM // 256, tile, 0)

    def stored_products():
        loads[6].wait()
        corr_h[...] = jnp.zeros_like(corr_h)

        def tile(t, carry):
            cols = pl.ds(pl.multiple_of(t * 128, 128), 128)
            vals = [err[k, :, cols].astype(F32) for k in range(5)]
            n = 0
            for i in range(5):
                for j in range(i + 1):
                    corr_h[n : n + 1, :] += jnp.sum(vals[i] * vals[j], axis=0, keepdims=True)
                    n += 1
            return carry

        lax.fori_loop(0, NT, tile, 0)

    def send_group(src_ref, dst_ref, k, count, to):
        def one(o, carry):
            remote(src_ref, dst_ref.at[o - 1], c_s.at[k], c_r.at[k], to(o)).start()
            return carry

        lax.fori_loop(1, count, one, 0)

    def wait_group(dst_ref, k):
        remote(dst_ref, dst_ref, c_s.at[k], c_r.at[k], twin).wait_recv()

    def wait_group_sent(dst_ref, k):
        remote(dst_ref, dst_ref, c_s.at[k], c_r.at[k], twin).wait_send()

    def to_col(o):
        return (row, (col + o) % COLS)

    def to_row(o):
        return ((row + o) % ROWS, col)

    def total_of(k, got):
        return sums[k] + jnp.sum(got[...], axis=0)

    eye = lax.broadcasted_iota(jnp.int32, (16, 128), 0) == lax.broadcasted_iota(jnp.int32, (16, 128), 1)

    def pack(values):
        tall = jnp.broadcast_to(jnp.sum(values, axis=1, keepdims=True), (16, 128))
        return jnp.sum(jnp.where(eye, tall, 0.0), axis=0, keepdims=True)

    def unpack(values):
        tall = jnp.where(eye, jnp.broadcast_to(values, (16, 128)), 0.0)
        return jnp.broadcast_to(jnp.sum(tall, axis=1, keepdims=True), (16, 128))

    def own_rows(p):
        n = rows_of(p)
        rows = slice(SUB * p, SUB * p + n)
        everything = z_in.at[p]
        remote(everything, everything, z_s.at[0], z_r.at[p], twin).wait_recv()
        scales = zs_in.at[p]
        remote(scales, scales, zs_s.at[0], zs_r.at[p], twin).wait_recv()

        def add(k, total):
            return total + decode(z_in[p, k], zs_in[p, k])

        ladder = lax.fori_loop(0, NZ - 1, add, z_own[p])[0:n]
        if p == 0:
            loads[7].wait()
            loads[8].wait()
            corr_n[...] = jnp.zeros_like(corr_n)
        gap = widen(up[rows, :], NT) - vq[0:1, :]
        raw = (src[rows, :] + ladder) / gap
        raw_buf[rows, :] = raw
        new = raw - amp[0, rows, :].astype(F32)
        for k in range(5):
            corr_n[k : k + 1, :] += lane_sums(new * err[k, rows, :].astype(F32))
        corr_n[5:6, :] += lane_sums(new * new)

    def greet_z(i):
        for far_z in ((z + 1 + i) % NZ, (z + NZ - 1 - i) % NZ):
            pl.semaphore_signal(greet.at[i], inc=1, device_id=(far_z * NX + x, col), device_id_type=MESH)

    pl.semaphore_wait(barrier, len(direct))
    greet_z(0)
    own_up[0].start()
    own_down[0].start()
    for p in range(PIECES):
        own_twin[p].start()
    for p in range(1, LEAD):
        own_up[p].start()
        own_down[p].start()

    def serve_near(p):
        own_up[p].wait_recv()
        fwd_up[p].start()
        near_twin[0][p].start()
        own_down[p].wait_recv()
        fwd_down[p].start()
        near_twin[1][p].start()
        if p + LEAD < PIECES:
            own_up[p + LEAD].start()
            own_down[p + LEAD].start()

    def serve_far(p):
        fwd_up[p].wait_recv()
        far_twin[0][p].start()
        fwd_down[p].wait_recv()
        far_twin[1][p].start()

    def arrived(g):
        kind, p, first, n = GROUP_LIST[g]
        if kind == "own":
            loads[1].wait()
        elif kind == "sib":
            for q in range(PIECES):
                own_twin[q].wait_recv()
        elif kind == "near" and first + n == 4:
            near_twin[0][p].wait_recv()
            near_twin[1][p].wait_recv()
        elif kind == "far" and first + n == 2:
            far_twin[0][p].wait_recv()
            far_twin[1][p].wait_recv()

    def run_multiply(g):
        arrived(g)
        multiply(g)
        stage_a(g)

    def greetings(i):
        pl.semaphore_wait(greet.at[i], 2)
        if i == 0:
            greet_z(1)

    def products(i):
        if i == 0:
            stored_products()
            sums[0] = pack(corr_h[...])
        elif i == 1:
            send_group(sums.at[0], h1_in, 0, COLS, to_col)
        else:
            wait_group(h1_in, 0)
            sums[1] = total_of(0, h1_in)
            send_group(sums.at[1], h2_in, 1, ROWS, to_row)

    steps = {
        "m": run_multiply, "b": stage_b, "c": stage_c, "d": own_rows, "s": serve_near,
        "f": serve_far, "k": greetings, "h": products, "e": lambda i: energies(),
    }
    for step in SEQUENCE:
        steps[step[0]](int(step[1:]))
    sums[2] = pack(corr_n[...])
    send_group(sums.at[2], n1_in, 2, COLS, to_col)
    for g in range(GROUPS):
        finish_sends(g)
    wait_group(n1_in, 2)
    sums[3] = total_of(2, n1_in)
    send_group(sums.at[3], n2_in, 3, ROWS, to_row)
    for group in [own_up, own_down, own_twin, fwd_up, fwd_down] + near_twin + far_twin:
        for copy in group:
            copy.wait_send()
    wait_group(h2_in, 1)
    stored = unpack(total_of(1, h2_in))
    for k, ref in enumerate((h1_in, h2_in, n1_in)):
        wait_group_sent(ref, k)
    wait_group(n2_in, 3)
    fresh = unpack(total_of(3, n2_in))
    corr = [[None] * 6 for _ in range(6)]
    n = 0
    for i in range(5):
        for j in range(i + 1):
            corr[i][j] = stored[n : n + 1, :]
            n += 1
    for j in range(6):
        corr[5][j] = fresh[j : j + 1, :]
    weights = [widen(w, NT) for w in solve(corr)]
    for p in range(PIECES):
        rows = slice(SUB * p, SUB * p + rows_of(p))
        total = weights[5] * raw_buf[rows, :]
        for k in range(5):
            total = total + weights[k] * amp[k, rows, :].astype(F32)
        out_ref[rows, :] = total
    wait_group_sent(n2_in, 3)


def on_device(integrals, lambda2, source_terms, hist_amp, hist_err, eps_occ, eps_vir, occ_pair, vir_pair):
    vmem = pltpu.VMEM
    dma = pltpu.SemaphoreType.DMA
    i16 = jnp.int16
    scratch = [
        vmem((KDIM, NDIM), BF16),
        vmem((252, KDIM), BF16),
        vmem((BLOCK, NDIM), F32),
        vmem((5, BLOCK, NDIM), BF16),
        vmem((5, BLOCK, NDIM), BF16),
        vmem((1, 64), F32),
        vmem((800,), F32),
        vmem((2, BLOCK), jnp.int32),
        vmem((2, NDIM), jnp.int32),
        vmem((256, KDIM), BF16),
        vmem((256, KDIM), BF16),
        vmem((PIECES, 256, KDIM), BF16),
        vmem((PIECES, 128, KDIM), BF16),
        vmem((UNITS, NX, SUB, NDIM), F32),
        vmem((2, UNITS, SUB, NDIM // 2), i16),
        vmem((2, UNITS, SUB, NDIM // 2), i16),
        vmem((2, UNITS, 1, 128), F32),
        vmem((2, UNITS, 1, 128), F32),
        vmem((2, UNITS, SUB, NDIM), i16),
        vmem((2, UNITS, SUB, NDIM), i16),
        vmem((2, UNITS, 1, 128), F32),
        vmem((2, UNITS, 1, 128), F32),
        vmem((UNITS, SUB, NDIM), i16),
        vmem((PIECES, NZ - 1, SUB, NDIM), i16),
        vmem((UNITS, 1, 128), F32),
        vmem((PIECES, NZ - 1, 1, 128), F32),
        vmem((PIECES, SUB, NDIM), F32),
        vmem((BLOCK, NDIM), F32),
        vmem((BLOCK, 128), F32),
        vmem((8, NDIM), F32),
        vmem((16, 128), F32),
        vmem((16, 128), F32),
        vmem((4, 1, 128), F32),
        vmem((COLS - 1, 1, 128), F32),
        vmem((ROWS - 1, 1, 128), F32),
        vmem((COLS - 1, 1, 128), F32),
        vmem((ROWS - 1, 1, 128), F32),
        pltpu.SemaphoreType.REGULAR((2,)),
        dma((9,)),
        dma((9 * PIECES,)),
        dma((9 * PIECES,)),
    ] + [dma((GROUPS, 2))] * 8 + [dma((UNITS,))] * 2 + [dma((PIECES,))] * 2 + [dma((4,))] * 2
    call = pl.pallas_call(
        kernel,
        out_shape=jax.ShapeDtypeStruct((BLOCK, NDIM), F32),
        in_specs=[pl.BlockSpec(memory_space=pltpu.HBM)] * 9,
        out_specs=pl.BlockSpec(memory_space=pltpu.VMEM),
        scratch_shapes=scratch,
        compiler_params=pltpu.CompilerParams(
            collective_id=0, has_side_effects=True, vmem_limit_bytes=44 * 1024 * 1024
        ),
        name="ladder",
    )
    operands = (
        integrals, lambda2, source_terms, hist_amp, hist_err,
        eps_occ.reshape(1, 64), eps_vir, occ_pair, vir_pair,
    )
    return call(*[pltpu.with_memory_space_constraint(o, pltpu.HBM) for o in operands])


def solution(mesh):
    placed = (
        P("row", "col"),
        P("col", "row"),
        P("row", "col"),
        P(None, "row", "col"),
        P(None, "row", "col"),
        P(),
        P(),
        P(None, "row"),
        P(None, "col"),
    )
    return jax.shard_map(
        on_device, mesh=mesh, in_specs=placed, out_specs=P("row", "col"), check_vma=False
    )
```
